32 devices in a mesh: dp: 4 (over y, x), vocab: 8 (over z, core).
Axes of the slice: x: 2, y: 2, z: 4, core: 2. Of those that a mesh axis runs over, the one named last changes fastest.
Arguments:
- final_activation: bfloat16 [512, 8192], P('dp', 'vocab'), may hold values from -2000 to 2000
- output_projection_weights: bfloat16 [8192, 128256], P('dp', 'vocab'), may hold values from -0.0625 to 0.0625
- context_word_tallies: int32 [512, 128256], P('dp', 'vocab'), may hold values from 0 to 2
- emitted_word_tallies: int32 [512, 128256], P('dp', 'vocab'), may hold values from 0 to 2
- freshest_word: int32 [512], P('dp'), may hold values from 0 to 128255
- recurrence_divisor: float32 [512], P('dp'), may hold values from 1.1 to 2.5
- recurrence_fine: float32 [512], P('dp'), may hold values from 0 to 1.5
- appearance_fine: float32 [512], P('dp'), may hold values from 0 to 1.5
- softness_level: float32 [512], P('dp'), may hold values from 0.5 to 2
- random_draws: float32 [512], P('dp'), may hold values from 0.02 to 0.98
Outputs:
- new_counts: int32 [512, 128256], P('dp', 'vocab')
- log_likelihoods: float32 [512, 128256], P('dp', 'vocab')
- sample_quantile: float32 [512], P('dp')
The draws below stay inside these ranges and needn't reach their ends.
All inputs are finite; a program needn't handle non-finite values.
Results may differ from the reference program's by a relative error of at most 0.0012.
Values may be sent and summed in bfloat16 or wider, within the bound.
A program may use at most 192 MiB of HBM per device.

```python
import math
import jax
import jax.numpy as jnp
from jax import lax

D = 8192
VOCAB = 128256
STREAM_NUMBER = 512
N_VOCAB = 8


def draw_final_activation(key, part):
    values = jnp.clip(jax.random.normal(key, (STREAM_NUMBER, D), jnp.float32), -6.0, 6.0)
    row_ids = lax.broadcasted_iota(jnp.int32, (STREAM_NUMBER, 1), 0)
    values = values * jnp.where(row_ids % 4 == 0, 150.0, 1.0)
    return values.astype(jnp.bfloat16)


def place_ends(array, own_key, smallest, largest):
    longest = array.shape.index(max(array.shape))
    spots = []
    for shift in (0, 1):
        where = [jax.random.randint(jax.random.fold_in(own_key, axis), (), 0, length) for axis, length in enumerate(array.shape)]
        where[longest] = (where[longest] + shift) % array.shape[longest]
        spots.append(tuple(where))
    return array.at[spots[0]].set(smallest).at[spots[1]].set(largest)


def shard_levels(own_key, dims, pieces, low, top_value):
    level, own = 1.0, jax.random.fold_in(own_key, 6)
    for dim, shards_of in pieces:
        draws = jnp.exp(jax.random.uniform(jax.random.fold_in(own, dim), (shards_of,), jnp.float32, low / len(pieces), top_value / len(pieces)))
        level = level * jnp.repeat(draws, dims[dim] // shards_of).reshape([-1 if axis == dim else 1 for axis in range(len(dims))])
    return level


def centred(key, dims, width, limit, pieces=(), kind=jnp.bfloat16):
    gain = shard_levels(key, dims, pieces, -0.22, 0.18) if pieces else 1.0
    entries = jax.random.normal(key, dims, jnp.float32) * width * gain
    return jnp.minimum(jnp.maximum(entries, -limit), limit).astype(kind)


def setup_inputs(seed: int = 0) -> dict:
    arg_keys = jax.random.split(jax.random.key(seed), 11)
    final_activation = draw_final_activation(jax.random.fold_in(arg_keys[10], 71), 0)
    output_projection_weights = centred(arg_keys[1], (D, VOCAB), D ** -0.5, 0.0625, ((0, 4), (1, 8)))
    context_word_tallies = place_ends(jax.random.randint(arg_keys[2], (STREAM_NUMBER, VOCAB), 0, 3), jax.random.fold_in(arg_keys[2], 1), 0, 2).astype(jnp.int32)
    emitted_word_tallies = place_ends(jax.random.randint(arg_keys[3], (STREAM_NUMBER, VOCAB), 0, 3), jax.random.fold_in(arg_keys[3], 1), 0, 2).astype(jnp.int32)
    freshest_word = place_ends(jax.random.randint(arg_keys[4], (STREAM_NUMBER,), 0, VOCAB), jax.random.fold_in(arg_keys[4], 1), 0, VOCAB - 1).astype(jnp.int32)
    recurrence_divisor = jnp.clip(jnp.exp(math.log(2.5) - 0.82098053 * jax.random.uniform(arg_keys[5], (STREAM_NUMBER,), jnp.float32) ** shard_levels(arg_keys[5], (STREAM_NUMBER,), ((0, 4),), -0.2, 0.2)), 1.1, 2.5)
    recurrence_fine = jnp.clip(1.5 * jax.random.uniform(arg_keys[6], (STREAM_NUMBER,), jnp.float32) ** shard_levels(arg_keys[6], (STREAM_NUMBER,), ((0, 4),), -0.2, 0.2), 0.0, 1.5)
    appearance_fine = jnp.clip(1.5 * jax.random.uniform(arg_keys[7], (STREAM_NUMBER,), jnp.float32) ** shard_levels(arg_keys[7], (STREAM_NUMBER,), ((0, 4),), -0.2, 0.2), 0.0, 1.5)
    softness_level = jnp.clip(jnp.exp(math.log(2.0) - 1.3862944 * jax.random.uniform(arg_keys[8], (STREAM_NUMBER,), jnp.float32) ** shard_levels(arg_keys[8], (STREAM_NUMBER,), ((0, 4),), -0.2, 0.2)), 0.5, 2.0)
    random_draws = jnp.clip(0.02 + 0.96000002 * jax.random.uniform(arg_keys[9], (STREAM_NUMBER,), jnp.float32) ** shard_levels(arg_keys[9], (STREAM_NUMBER,), ((0, 4),), -0.2, 0.2), 0.02, 0.98)
    return dict(final_activation=final_activation, output_projection_weights=output_projection_weights, context_word_tallies=context_word_tallies, emitted_word_tallies=emitted_word_tallies, freshest_word=freshest_word, recurrence_divisor=recurrence_divisor, recurrence_fine=recurrence_fine, appearance_fine=appearance_fine, softness_level=softness_level, random_draws=random_draws)


def reference(final_activation, output_projection_weights, context_word_tallies, emitted_word_tallies, freshest_word, recurrence_divisor, recurrence_fine, appearance_fine, softness_level, random_draws):
    block_width = VOCAB // N_VOCAB
    hidden_wide = final_activation.astype(jnp.float32)

    def one_block(index):
        weight_block = lax.dynamic_slice_in_dim(output_projection_weights, index * block_width, block_width, 1).astype(jnp.float32)
        return jnp.dot(hidden_wide, weight_block, preferred_element_type=jnp.float32, precision=lax.Precision.HIGHEST)

    blocks = lax.map(one_block, jnp.arange(N_VOCAB, dtype=jnp.int32))
    logits = jnp.transpose(blocks, (1, 0, 2)).reshape(final_activation.shape[0], VOCAB)
    token_ids = jnp.arange(VOCAB, dtype=jnp.int32)
    new_counts = emitted_word_tallies + (token_ids[None, :] == freshest_word[:, None]).astype(jnp.int32)
    seen = (context_word_tallies + new_counts) > 0
    factor = recurrence_divisor[:, None]
    adjusted_scores = jnp.where(seen, jnp.where(logits > 0, logits / factor, logits * factor), logits)
    adjusted_scores = adjusted_scores - recurrence_fine[:, None] * new_counts.astype(jnp.float32)
    adjusted_scores = adjusted_scores - appearance_fine[:, None] * (new_counts > 0).astype(jnp.float32)
    softened_scores = adjusted_scores / softness_level[:, None]
    highest_score = jnp.max(softened_scores, axis=1, keepdims=True)
    exponentiated_mass = jnp.exp(softened_scores - highest_score)
    normalizer_mass = jnp.sum(exponentiated_mass, axis=1, keepdims=True)
    log_likelihoods = softened_scores - highest_score - jnp.log(normalizer_mass)
    probs = exponentiated_mass / normalizer_mass
    cdf = jnp.cumsum(probs, axis=1)
    below = cdf - probs
    taken = jnp.minimum(jnp.maximum(random_draws[:, None] - below, 0.0), probs)
    position = (token_ids.astype(jnp.float32) + 0.5) / VOCAB
    sample_quantile = jnp.sum(taken * position[None, :], axis=1)
    return new_counts, log_likelihoods, sample_quantile
```

```python
import functools

import jax
import jax.numpy as jnp
from jax import lax
from jax.experimental import pallas as pl
from jax.experimental.pallas import tpu as pltpu
from jax.sharding import PartitionSpec as P

ROWS = 512
TILE = 128
FINISH_ROWS = 1024
LOWEST = -1e30
SHARES = (5, 11, 11, 5)


def spans(width):
    blocks = pl.cdiv(width, ROWS)
    total, edges, seen = sum(SHARES), [0], 0
    for share in SHARES:
        seen += share
        edge = min(blocks, -(-blocks * seen // total))
        if edge > edges[-1]:
            edges.append(edge)
    return [(low, high) for low, high in zip(edges[:-1], edges[1:])]


def penalize_kernel(
    first_block, width, begins, logits, context, emitted, newest, numbers, *rest
):
    if not begins:
        stats_in, _, _, *rest = rest
    scores, counts, stats = rest
    step = pl.program_id(0)

    @pl.when(step == 0)
    def _():
        if begins:
            stats[0:1, :] = jnp.full_like(stats[0:1, :], LOWEST)
            stats[1:2, :] = jnp.zeros_like(stats[1:2, :])
            stats[2:8, :] = jnp.zeros_like(stats[2:8, :])
        else:
            stats[...] = stats_in[...]

    place = (first_block + step) * ROWS + lax.broadcasted_iota(jnp.int32, (ROWS, TILE), 0)
    first_id = lax.axis_index("vocab") * width
    new_counts = emitted[...] + jnp.where(place + first_id == newest[...], 1, 0)
    counts[...] = new_counts
    raw = logits[...]
    divisor, inverse = numbers[0:1, :], numbers[1:2, :]
    frequency, presence, cooling = numbers[2:3, :], numbers[3:4, :], numbers[4:5, :]
    scale = jnp.where(raw > 0, inverse, divisor)
    value = jnp.where(context[...] + new_counts > 0, raw * scale, raw)
    value = value - frequency * new_counts.astype(jnp.float32)
    value = value - jnp.where(new_counts > 0, presence, 0.0)
    value = value * cooling
    scores[...] = value
    value = jnp.where(place < width, value, LOWEST)
    before = stats[0:1, :]
    highest = jnp.maximum(before, jnp.max(value, axis=0, keepdims=True))
    mass = jnp.sum(jnp.exp(value - highest), axis=0, keepdims=True)
    stats[1:2, :] = stats[1:2, :] * jnp.exp(before - highest) + mass
    stats[0:1, :] = highest


def penalize(low, high, width, logits, context, emitted, newest, numbers, carried):
    lanes = logits.shape[1]
    begins = carried is None
    own = pl.BlockSpec((ROWS, lanes), lambda i: (i, 0))
    shifted = pl.BlockSpec((ROWS, lanes), lambda i: (low + i, 0))
    small = pl.BlockSpec((8, lanes), lambda i: (0, 0))
    line = pl.BlockSpec((1, lanes), lambda i: (0, 0))
    in_specs = [own, shifted, shifted, line, small]
    operands = [logits, context, emitted, newest, numbers]
    aliases = {}
    if not begins:
        anywhere = pl.BlockSpec(memory_space=pl.ANY)
        scores, counts, stats = carried
        in_specs += [small, anywhere, anywhere]
        operands += [stats, scores, counts]
        aliases = {6: 0, 7: 1}
    rows = (high - low) * ROWS
    return pl.pallas_call(
        functools.partial(penalize_kernel, low, width, begins),
        grid=(high - low,),
        in_specs=in_specs,
        out_specs=[shifted, shifted, small],
        out_shape=[
            jax.ShapeDtypeStruct((width, lanes), jnp.float32),
            jax.ShapeDtypeStruct((width, lanes), jnp.int32),
            jax.ShapeDtypeStruct((8, lanes), jnp.float32),
        ],
        input_output_aliases=aliases,
        compiler_params=pltpu.CompilerParams(
            dimension_semantics=("arbitrary",)
        ),
        cost_estimate=pl.CostEstimate(
            flops=rows * lanes * 40,
            bytes_accessed=rows * lanes * 20,
            transcendentals=rows * lanes,
        ),
    )(*operands)


def finish_kernel(width, shards, scores, gathered, draws, likelihoods, quantile, held):
    step = pl.program_id(0)
    own = lax.axis_index("vocab")
    lanes = scores.shape[1]

    @pl.when(step == 0)
    def _():
        highest = gathered[0:1, :]
        for shard in range(1, shards):
            highest = jnp.maximum(highest, gathered[8 * shard : 8 * shard + 1, :])
        total = jnp.zeros_like(highest)
        lower = jnp.zeros_like(highest)
        for shard in range(shards):
            own_highest = gathered[8 * shard : 8 * shard + 1, :]
            mass = gathered[8 * shard + 1 : 8 * shard + 2, :] * jnp.exp(own_highest - highest)
            total = total + mass
            lower = lower + jnp.where(shard < own, mass, 0.0)
        held[0:1, :] = highest
        held[1:2, :] = jnp.log(total)
        held[2:3, :] = lower / total
        quantile[...] = jnp.zeros_like(quantile)

    highest, log_total = held[0:1, :], held[1:2, :]
    draw = draws[...]
    carry = held[2:3, :]
    row = lax.broadcasted_iota(jnp.int32, (TILE, TILE), 0)
    column = lax.broadcasted_iota(jnp.int32, (TILE, TILE), 1)
    strictly_lower = jnp.where(row > column, 1.0, 0.0).astype(jnp.bfloat16)
    spot = lax.broadcasted_iota(jnp.int32, (TILE, lanes), 0)
    first_id = own * width
    gained = jnp.zeros((8, lanes), jnp.float32)
    for tile in range(FINISH_ROWS // TILE):
        base = step * FINISH_ROWS + tile * TILE
        window = slice(tile * TILE, (tile + 1) * TILE)
        value = (scores[window, :] - highest) - log_total
        likelihoods[window, :] = value
        prob = jnp.where(spot < width - base, jnp.exp(value), 0.0)
        below = carry
        left = prob
        for _ in range(3):
            piece = left.astype(jnp.bfloat16)
            left = left - piece.astype(jnp.float32)
            below = below + jnp.dot(
                strictly_lower, piece, preferred_element_type=jnp.float32
            )
        taken = jnp.minimum(jnp.maximum(draw - below, 0.0), prob)
        position = ((spot + (base + first_id)).astype(jnp.float32) + 0.5) * (
            1.0 / (width * shards)
        )
        gained = gained + jnp.sum((taken * position).reshape(TILE // 8, 8, lanes), axis=0)
        carry = carry + jnp.sum(prob, axis=0, keepdims=True)
    held[2:3, :] = carry
    quantile[...] += gained


def finish(scores, gathered, draws, shards):
    width, lanes = scores.shape
    block = pl.BlockSpec((FINISH_ROWS, lanes), lambda i: (i, 0))
    return pl.pallas_call(
        functools.partial(finish_kernel, width, shards),
        grid=(pl.cdiv(width, FINISH_ROWS),),
        in_specs=[
            block,
            pl.BlockSpec((8 * shards, lanes), lambda i: (0, 0)),
            pl.BlockSpec((1, lanes), lambda i: (0, 0)),
        ],
        out_specs=[block, pl.BlockSpec((8, lanes), lambda i: (0, 0))],
        out_shape=[
            jax.ShapeDtypeStruct((width, lanes), jnp.float32),
            jax.ShapeDtypeStruct((8, lanes), jnp.float32),
        ],
        scratch_shapes=[pltpu.VMEM((8, lanes), jnp.float32)],
        compiler_params=pltpu.CompilerParams(
            dimension_semantics=("arbitrary",)
        ),
        cost_estimate=pl.CostEstimate(
            flops=width * lanes * 40,
            bytes_accessed=width * lanes * 8,
            transcendentals=width * lanes,
        ),
    )(scores, gathered, draws)


def quarter_of_features(hidden):
    shards, groups = lax.axis_size("vocab"), lax.axis_size("dp")
    pairs = shards // 2
    same_core = [[core + 2 * pair for pair in range(pairs)] for core in range(2)]
    full_rows = lax.all_gather(
        hidden, "vocab", axis=1, tiled=True, axis_index_groups=same_core
    )
    own = lax.all_to_all(full_rows, "dp", split_axis=1, concat_axis=0, tiled=True)
    other = lax.ppermute(own, "vocab", [(index, index ^ 1) for index in range(shards)])
    shape = (own.shape[0], pairs // groups, 1, hidden.shape[1])
    own, other = own.reshape(shape), other.reshape(shape)
    joined = jnp.where(
        lax.axis_index("vocab") % 2 == 0,
        jnp.concatenate([own, other], 2),
        jnp.concatenate([other, own], 2),
    )
    return joined.reshape(own.shape[0], -1)


def on_device(
    final_activation,
    output_projection_weights,
    context_word_tallies,
    emitted_word_tallies,
    freshest_word,
    recurrence_divisor,
    recurrence_fine,
    appearance_fine,
    softness_level,
    random_draws,
):
    shards = lax.axis_size("vocab")
    width = output_projection_weights.shape[1]
    quarter_rows = quarter_of_features(final_activation)
    numbers = jnp.stack(
        [
            recurrence_divisor,
            1.0 / recurrence_divisor,
            recurrence_fine,
            appearance_fine,
            1.0 / softness_level,
        ]
        + [jnp.zeros_like(softness_level)] * 3
    )
    newest = freshest_word[None, :]
    context, emitted = context_word_tallies.T, emitted_word_tallies.T
    pieces = []
    for low, high in spans(width):
        weights = output_projection_weights[:, low * ROWS : min(high * ROWS, width)]
        share = jnp.dot(quarter_rows, weights, preferred_element_type=jnp.float32)
        pieces.append(
            lax.psum_scatter(share, "dp", scatter_dimension=0, tiled=True)
        )
    carried = None
    for (low, high), piece in zip(spans(width), pieces):
        carried = penalize(
            low, high, width, piece.T, context, emitted, newest, numbers, carried
        )
    scores, new_counts, stats = carried
    gathered = lax.all_gather(stats, "vocab", axis=0, tiled=True)
    likelihoods, parts = finish(scores, gathered, random_draws[None, :], shards)
    part = jnp.sum(parts, axis=0, keepdims=True)
    sample_quantile = jnp.sum(lax.all_gather(part, "vocab", axis=0, tiled=True), axis=0)
    return (new_counts.T, likelihoods.T, sample_quantile)


def solution(mesh):
    return jax.shard_map(
        on_device,
        mesh=mesh,
        in_specs=(
            P("dp", "vocab"),
            P("dp", "vocab"),
            P("dp", "vocab"),
            P("dp", "vocab"),
            P("dp"),
            P("dp"),
            P("dp"),
            P("dp"),
            P("dp"),
            P("dp"),
        ),
        out_specs=(P("dp", "vocab"), P("dp", "vocab"), P("dp")),
        check_vma=False,
    )
```
